32 devices in a mesh: gx: 4 (over z), gy: 2 (over y), gz: 4 (over x, core).
Axes of the slice: x: 2, y: 2, z: 4, core: 2. Of those that a mesh axis runs over, the one named last changes fastest.
Arguments:
- positions: float32 [3, 16, 8, 512], P(None, 'gx', 'gy', 'gz'), may hold values from 0.6 to 13.9, as said below
- counts: int32 [16, 8, 8], P('gx', 'gy', 'gz'), may hold values from 24 to 64
Outputs:
- forces: float32 [3, 16, 8, 512], P(None, 'gx', 'gy', 'gz')
- energy: float32 [16, 8, 512], P('gx', 'gy', 'gz')
The draws below stay inside these ranges and needn't reach their ends.
Inputs may be any that keep to these rules, and one draw needn't show every extreme that they name: `positions`: each cell is a box of 2a x 2a x 4a with a = 3.615 and every atom lies inside its own cell's box; two atoms are 1.0 or more apart, and no atom is within 5.51 of an atom outside its cell's 27 neighbour cells.
All inputs are finite; a program needn't handle non-finite values.
Results may differ from the reference program's by a relative error of at most 0.0003.
Values sent between devices are 32-bit elements; how exact they have to be, the bound alone decides.
A program may use at most 64 MiB of HBM per device.

```python
import jax
import jax.numpy as jnp
from jax import lax

CX = 4
SLOTS = 64
NX = 16
NY = 8
NZ = 8
N_GX = 4


lattice_const = 3.615


def site_table():
    site_index = jnp.arange(64, dtype=jnp.int32)
    basis_id = site_index % 4
    unit_id = site_index // 4
    unit_x = (unit_id % 2).astype(jnp.float32)
    unit_y = (unit_id // 2 % 2).astype(jnp.float32)
    unit_z = (unit_id // 4).astype(jnp.float32)
    half_x = jnp.where((basis_id == 2) | (basis_id == 3), 0.5, 0.0)
    half_y = jnp.where((basis_id == 1) | (basis_id == 3), 0.5, 0.0)
    half_z = jnp.where((basis_id == 1) | (basis_id == 2), 0.5, 0.0)
    return jnp.stack([unit_x + half_x + 0.25, unit_y + half_y + 0.25, unit_z + half_z + 0.25]) * lattice_const


def permute_slots(cell_key):
    return jax.random.permutation(cell_key, 64)[:SLOTS]


def draw_positions(key, part):
    cell_count = NX * NY * NZ
    cell_keys = jax.random.split(jax.random.fold_in(key, 7), cell_count)
    chosen = jax.vmap(permute_slots)(cell_keys)
    base = site_table()[:, chosen]
    noise_key = jax.random.fold_in(key, 8)
    jitter = jnp.clip(0.08 * jax.random.normal(noise_key, (3, cell_count, SLOTS), jnp.float32), -0.25, 0.25)
    placed = base + jitter
    reach = jax.random.uniform(jax.random.fold_in(key, 9), (cell_count,), jnp.float32, 1.0, 1.15)
    chosen_cells = jax.random.randint(jax.random.fold_in(key, 10), (cell_count,), 0, 2) == 1
    heading = jnp.where(base[0, :, 0] > lattice_const, -1.0, 1.0)
    zeros_row = jnp.zeros((cell_count,), jnp.float32)
    moved = placed[:, :, 0] + jnp.stack([heading * reach, zeros_row, zeros_row])
    second = jnp.where(chosen_cells[None, :], moved, placed[:, :, 1])
    placed = jnp.concatenate([placed[:, :, :1], second[:, :, None], placed[:, :, 2:]], axis=2)
    return placed.reshape(3, NX, NY, NZ * SLOTS).astype(jnp.float32)


def touch_ends(values, own_key, low, high):
    place = [jax.random.randint(jax.random.fold_in(own_key, axis), (), 0, length) for axis, length in enumerate(values.shape)]
    main_axis = values.shape.index(max(values.shape))
    neighbour = place[:main_axis] + [(place[main_axis] + 1) % values.shape[main_axis]] + place[main_axis + 1:]
    return values.at[tuple(place)].set(low).at[tuple(neighbour)].set(high)


def setup_inputs(seed: int = 0) -> dict:
    streams_of = jax.random.split(jax.random.key(seed), 3)
    positions = draw_positions(jax.random.fold_in(streams_of[2], 71), 0)
    counts = touch_ends(jax.random.randint(streams_of[1], (NX, NY, NZ), SLOTS * 3 // 8, SLOTS + 1), jax.random.fold_in(streams_of[1], 1), SLOTS * 3 // 8, SLOTS).astype(jnp.int32)
    return dict(positions=positions, counts=counts)


lattice_const = 3.615
cell_span = (2.0 * lattice_const, 2.0 * lattice_const, 4.0 * lattice_const)
cut_radius = 5.50679
cut_width = 0.50037
dens_scale = 3.80362
beta_one = 0.17394
radius_three = -2.19885
energy_one = 201.458
energy_two = 0.00659288
radius_one = 0.83591
radius_two = 4.46867
alpha_one = 2.97758
alpha_two = 1.54927
shift_delta = 0.0086225
repulsion = ((4.0, 2.24), (40.0, 1.8), (1150.0, 1.2))
embed_zero = -2.28235
embed_curve = 1.35535
lower_terms = (-1.27775, -0.86074, 1.78804, 2.97571)
upper_quartic = 0.4
upper_damping = 0.3
cell_offsets = [(first, second, third) for first in (-1, 0, 1) for second in (-1, 0, 1) for third in (-1, 0, 1)]

def tapering(radius):
    scaled = (radius - cut_radius) / cut_width
    quartic = scaled ** 4
    inside = scaled < 0.0
    taper_value = jnp.where(inside, quartic / (1.0 + quartic), 0.0)
    taper_slope = jnp.where(inside, 4.0 * scaled ** 3 / (1.0 + quartic) ** 2 / cut_width, 0.0)
    return (taper_value, taper_slope)

def gaussian_part(radius):
    return dens_scale * jnp.exp(-beta_one * (radius - radius_three) ** 2)

def radial_density(radius):
    taper_value, taper_slope = tapering(radius)
    return gaussian_part(radius) * taper_value

def morse_terms(radius, center_at, stiffness):
    decay = jnp.exp(-stiffness * (radius - center_at))
    return (decay * decay - 2.0 * decay, 2.0 * stiffness * (decay - decay * decay))

def pair_terms(radius):
    taper_value, taper_slope = tapering(radius)
    gaussian = gaussian_part(radius)
    dens_value = gaussian * taper_value
    dens_slope = gaussian * (-2.0 * beta_one * (radius - radius_three)) * taper_value + gaussian * taper_slope
    morse_first, slope_first = morse_terms(radius, radius_one, alpha_one)
    morse_second, slope_second = morse_terms(radius, radius_two, alpha_two)
    base_value = energy_one * morse_first + energy_two * morse_second + shift_delta
    base_slope = energy_one * slope_first + energy_two * slope_second
    pair_value = base_value * taper_value
    pair_slope = base_slope * taper_value + base_value * taper_slope
    for strength, reach_at in repulsion:
        closeness = jnp.maximum(reach_at - radius, 0.0)
        pair_value = pair_value - strength * closeness ** 4
        pair_slope = pair_slope + 4.0 * strength * closeness ** 3
    return (pair_value, pair_slope, dens_value, dens_slope)

def embedding(density):
    excess = density - 1.0
    below_value = embed_zero + 0.5 * embed_curve * excess ** 2 + lower_terms[0] * excess ** 3 + lower_terms[1] * excess ** 4 + lower_terms[2] * excess ** 5 + lower_terms[3] * excess ** 6
    below_slope = embed_curve * excess + 3.0 * lower_terms[0] * excess ** 2 + 4.0 * lower_terms[1] * excess ** 3 + 5.0 * lower_terms[2] * excess ** 4 + 6.0 * lower_terms[3] * excess ** 5
    numerator = embed_zero + 0.5 * embed_curve * excess ** 2 + lower_terms[0] * excess ** 3 + upper_quartic * excess ** 4
    numer_slope = embed_curve * excess + 3.0 * lower_terms[0] * excess ** 2 + 4.0 * upper_quartic * excess ** 3
    denominator = 1.0 + upper_damping * excess ** 3
    above_value = numerator / denominator
    above_slope = (numer_slope * denominator - numerator * 3.0 * upper_damping * excess ** 2) / denominator ** 2
    is_below = excess < 0.0
    return (jnp.where(is_below, below_value, above_value), jnp.where(is_below, below_slope, above_slope))

def pair_geometry(center, beside, offset):
    displace = []
    for component in range(3):
        displace.append(beside[component][..., None, :] + offset[component] * cell_span[component] - center[component][..., :, None])
    weight = center[3][..., :, None] * beside[3][..., None, :]
    if offset == (0, 0, 0):
        slot_count = center.shape[-1]
        weight = weight * (1.0 - jnp.eye(slot_count, dtype=jnp.float32))
    squared = displace[0] ** 2 + displace[1] ** 2 + displace[2] ** 2
    radius = jnp.sqrt(jnp.where(weight > 0.0, squared, 100.0))
    return (displace, weight, radius)

def shifted_cells(view_data, offset, extent):
    return view_data[:, 1 + offset[0]:1 + offset[0] + extent[0], 1 + offset[1]:1 + offset[1] + extent[1], 1 + offset[2]:1 + offset[2] + extent[2]]

def cell_density(view_data):
    extent = (view_data.shape[1] - 2, view_data.shape[2] - 2, view_data.shape[3] - 2)
    center = view_data[:, 1:-1, 1:-1, 1:-1]
    summed = jnp.zeros(center.shape[1:], jnp.float32)
    for offset in cell_offsets:
        beside = shifted_cells(view_data, offset, extent)
        displace, weight, radius = pair_geometry(center, beside, offset)
        summed = summed + lax.optimization_barrier(jnp.sum(weight * radial_density(radius), axis=-1))
    return summed

def cell_forces(view_data, slope_data):
    extent = (view_data.shape[1] - 2, view_data.shape[2] - 2, view_data.shape[3] - 2)
    center = view_data[:, 1:-1, 1:-1, 1:-1]
    slope_center = slope_data[0, 1:-1, 1:-1, 1:-1]
    force_sums = [jnp.zeros(center.shape[1:], jnp.float32) for component in range(3)]
    pair_sum = jnp.zeros(center.shape[1:], jnp.float32)
    for offset in cell_offsets:
        beside = shifted_cells(view_data, offset, extent)
        slope_beside = shifted_cells(slope_data, offset, extent)[0]
        displace, weight, radius = pair_geometry(center, beside, offset)
        pair_value, pair_slope, dens_value, dens_slope = pair_terms(radius)
        factor = weight * (pair_slope + (slope_center[..., :, None] + slope_beside[..., None, :]) * dens_slope) / radius
        force_sums = [force_sums[component] + lax.optimization_barrier(jnp.sum(factor * displace[component], axis=-1)) for component in range(3)]
        pair_sum = pair_sum + lax.optimization_barrier(jnp.sum(weight * pair_value, axis=-1))
    return (jnp.stack(force_sums), pair_sum)

def reference(positions, counts):
    occupied = (jnp.arange(SLOTS, dtype=jnp.int32)[None, None, None, :] < counts[..., None]).astype(jnp.float32)
    coords = positions.reshape(3, NX, NY, NZ, SLOTS)
    packed = jnp.concatenate([coords, occupied[None]], axis=0)
    borders = ((0, 0), (1, 1), (1, 1), (1, 1), (0, 0))
    wrapped = jnp.pad(packed, borders, mode='wrap')
    starts = (jnp.arange(N_GX, dtype=jnp.int32) * CX).astype(jnp.int32)
    index_zero = jnp.zeros((), jnp.int32)

    def density_block(first_cell):
        view_data = lax.dynamic_slice(wrapped, (index_zero, first_cell, index_zero, index_zero, index_zero), (4, CX + 2, NY + 2, NZ + 2, SLOTS))
        return cell_density(view_data)
    density = lax.map(density_block, starts).reshape(NX, NY, NZ, SLOTS)
    embed_value, embed_slope = embedding(density)
    slope = embed_slope * occupied
    slope_wrapped = jnp.pad(slope[None], borders, mode='wrap')

    def force_block(first_cell):
        view_data = lax.dynamic_slice(wrapped, (index_zero, first_cell, index_zero, index_zero, index_zero), (4, CX + 2, NY + 2, NZ + 2, SLOTS))
        slope_data = lax.dynamic_slice(slope_wrapped, (index_zero, first_cell, index_zero, index_zero, index_zero), (1, CX + 2, NY + 2, NZ + 2, SLOTS))
        return cell_forces(view_data, slope_data)
    force_blocks, pair_blocks = lax.map(force_block, starts)
    forces = jnp.moveaxis(force_blocks, 1, 0).reshape(3, NX, NY, NZ * SLOTS)
    pair_sum = pair_blocks.reshape(NX, NY, NZ, SLOTS)
    energy = (occupied * (embed_value + 0.5 * pair_sum)).reshape(NX, NY, NZ * SLOTS)
    return (forces, energy)
```

```python
import functools
import math

import jax
import jax.numpy as jnp
from jax import lax
from jax.experimental import pallas as pl
from jax.experimental.pallas import tpu as pltpu
from jax.sharding import PartitionSpec as P

SLOTS = 64
LANES = 128
FAR = 1.0e4

lattice_const = 3.615
cell_span = (2.0 * lattice_const, 2.0 * lattice_const, 4.0 * lattice_const)
cut_radius = 5.50679
cut_width = 0.50037
dens_scale = 3.80362
beta_one = 0.17394
radius_three = -2.19885
energy_one = 201.458
energy_two = 0.00659288
radius_one = 0.83591
radius_two = 4.46867
alpha_one = 2.97758
alpha_two = 1.54927
shift_delta = 0.0086225
repulsion = ((4.0, 2.24), (40.0, 1.8), (1150.0, 1.2))
embed_zero = -2.28235
embed_curve = 1.35535
lower_terms = (-1.27775, -0.86074, 1.78804, 2.97571)
upper_quartic = 0.4
upper_damping = 0.3
LOG2E = math.log2(math.e)
KEEP_SQUARED = 5.5075**2
ROWS = 16
WIDE = 2


def embedding(density):
    excess = density - 1.0
    square = excess * excess
    cube = square * excess
    below_value = embed_zero + square * (
        0.5 * embed_curve
        + excess
        * (lower_terms[0] + excess * (lower_terms[1] + excess * (lower_terms[2] + excess * lower_terms[3])))
    )
    below_slope = excess * (
        embed_curve
        + excess
        * (
            3.0 * lower_terms[0]
            + excess * (4.0 * lower_terms[1] + excess * (5.0 * lower_terms[2] + excess * 6.0 * lower_terms[3]))
        )
    )
    numerator = embed_zero + square * (0.5 * embed_curve + excess * (lower_terms[0] + excess * upper_quartic))
    numer_slope = excess * (embed_curve + excess * (3.0 * lower_terms[0] + excess * 4.0 * upper_quartic))
    is_below = excess < 0.0
    denominator = jnp.where(is_below, 1.0, 1.0 + upper_damping * cube)
    above_value = numerator / denominator
    above_slope = (numer_slope - above_value * (3.0 * upper_damping) * square) / denominator
    return (
        jnp.where(is_below, below_value, above_value),
        jnp.where(is_below, below_slope, above_slope),
    )


def iota(shape, dim):
    return lax.broadcasted_iota(jnp.int32, shape, dim)


def compress_cell(halo_ref, cx, cy, cz, ny):
    shape = (8, LANES)
    row = iota(shape, 0)
    lane = iota(shape, 1)
    comp = row // 2
    odd = row % 2
    layer = jnp.where(odd == 0, jnp.where(lane < SLOTS, 0, 1), jnp.where(lane < SLOTS, 2, -1))
    is_x, is_y, is_z = (comp == 0, comp == 1, comp == 2)
    add_z = jnp.where(is_z, (layer - cz).astype(jnp.float32) * cell_span[2], 0.0)
    span = jnp.where(is_z, cell_span[2], jnp.where(is_y, cell_span[1], cell_span[0]))
    counted = comp < 3
    data, drops = ([], [])
    for o1 in (-1, 0, 1):
        for o2 in (-1, 0, 1):
            add = jnp.where(is_x, o1 * cell_span[0], jnp.where(is_y, o2 * cell_span[1], add_z))
            value = halo_ref[(cx + 1 + o1) * ny + cy + 1 + o2] + add
            gap = jnp.maximum(jnp.maximum(-value, value - span), 0.0)
            gap = jnp.where(counted, gap * gap, 0.0)
            gap = gap + pltpu.roll(gap, 4, 0)
            gap = gap + pltpu.roll(gap, 2, 0)
            data.append(value)
            drops.append(gap >= KEEP_SQUARED)
    dropped = jnp.concatenate([jnp.where(d, 1.0, 0.0) for d in drops], axis=0).astype(jnp.bfloat16)
    pre = jnp.where(iota((LANES, 2 * LANES), 1) >= LANES, 1.0, 0.0)
    pre = jnp.where(iota((LANES, 2 * LANES), 0) < iota((LANES, 2 * LANES), 1), 1.0, pre)
    sums = jnp.dot(dropped, pre.astype(jnp.bfloat16), preferred_element_type=jnp.float32)
    sums = sums.astype(jnp.int32)
    outs = []
    counts = jnp.zeros((1, LANES), jnp.int32)
    one_row = iota((1, LANES), 1)
    for k in range(9):
        value = data[k]
        move = jnp.where(drops[k], 0, sums[8 * k : 8 * k + 8, :LANES])
        for bit in range(7):
            step = 1 << bit
            value_in = pltpu.roll(value, LANES - step, 1)
            move_in = pltpu.roll(move, LANES - step, 1)
            comes = (move_in & step) != 0
            value = jnp.where(comes, value_in, value)
            move = jnp.where(comes, move_in, jnp.where((move & step) != 0, 0, move))
        outs.append(value)
        total = LANES - sums[8 * k : 8 * k + 8, LANES:]
        counts = jnp.where(one_row == 2 * k, total[0:1], counts)
        counts = jnp.where(one_row == 2 * k + 1, total[1:2], counts)
    return outs, counts


def merge_cell(packed_ref, count_ref, list_ref, cell):
    lane = iota((8, LANES), 1)
    offset = jnp.int32(0)
    current = jnp.zeros((8, LANES), jnp.float32)
    for k in range(18):
        number = count_ref[cell, k]
        tile = offset // LANES
        place = offset % LANES
        turned = pltpu.roll(packed_ref[cell * 18 + k], place, 1)
        current = jnp.where(lane >= place, turned, current)
        list_ref[tile] = current
        current = jnp.where(lane < place + number - LANES, turned, current)
        offset = offset + number
    tile = offset // LANES
    place = offset % LANES
    list_ref[tile] = jnp.where(lane >= place, FAR, current)
    for extra in range(1, WIDE):
        list_ref[tile + extra] = jnp.full((8, LANES), FAR, jnp.float32)
    return (offset + WIDE * LANES - 1) // (WIDE * LANES)


def taper_parts(radius):
    scaled = jnp.minimum(radius * (1.0 / cut_width) - cut_radius / cut_width, 0.0)
    square = scaled * scaled
    quartic = square * square
    inverse = pl.reciprocal(1.0 + quartic, approx=False)
    return scaled, square, quartic * inverse, inverse


def gaussian(radius):
    scale = math.sqrt(beta_one * LOG2E)
    along = radius * scale - radius_three * scale
    return along, jnp.exp2(math.log2(dens_scale) - along * along)


def pair_body(kind, centers, slope_i, tile):
    d = [tile[2 * c : 2 * c + 1] - centers[c] for c in range(3)]
    squared = d[0] * d[0] + d[1] * d[1] + d[2] * d[2]
    squared = jnp.where(squared < 0.25, 100.0, squared)
    inv = lax.rsqrt(squared)
    radius = squared * inv
    scaled, square, taper, inverse = taper_parts(radius)
    along, gauss = gaussian(radius)
    if kind == 0:
        return [gauss * taper]
    taper_slope = (square * scaled) * (inverse * inverse) * (4.0 / cut_width)
    scale = math.sqrt(beta_one * LOG2E)
    dens_slope = gauss * (taper_slope - (along * (2.0 * beta_one / scale)) * taper)
    u = jnp.exp2(radius * (-alpha_one * LOG2E) + alpha_one * LOG2E * radius_one)
    v = jnp.exp2(radius * (-alpha_two * LOG2E) + alpha_two * LOG2E * radius_two)
    a = u * u - u
    b = v * v - v
    base = energy_one * (a - u) + (energy_two * (b - v) + shift_delta)
    base_slope = (-2.0 * alpha_one * energy_one) * a + (-2.0 * alpha_two * energy_two) * b
    pair_value = base * taper
    pair_slope = base_slope * taper + base * taper_slope
    quarter = None
    for strength, reach in repulsion:
        close = jnp.maximum(reach - radius, 0.0)
        cubed = (4.0 * strength) * (close * close * close)
        pair_slope = pair_slope + cubed
        quarter = cubed * close if quarter is None else quarter + cubed * close
    pair_value = pair_value - 0.25 * quarter
    factor = (pair_slope + (slope_i + tile[6:7]) * dens_slope) * inv
    return [pair_value, factor * d[0], factor * d[1], factor * d[2]]


def fold(value):
    total = value[:, :LANES]
    for k in range(1, WIDE):
        total = total + value[:, k * LANES : (k + 1) * LANES]
    return total


def pair_kernel(kind, dims, *refs):
    if kind == 0:
        own_ref, halo_ref, embed_ref, slope_ref = refs[:4]
        rest = refs[4:]
    else:
        own_ref, halo_ref, embed_ref, force_ref, energy_ref = refs[:5]
        rest = refs[5:]
    packed_ref, count_vmem, count_ref, list_ref, column_ref, sum_ref, sem = rest
    cells_x, cells_y = dims
    columns = cells_x * cells_y
    cells = 2 * columns
    ny = cells_y + 2
    number = 1 if kind == 0 else 4

    @pl.loop(0, cells)
    def _(cell):
        column = cell // 2
        outs, counts = compress_cell(halo_ref, column // cells_y, column % cells_y, cell % 2, ny)
        for k in range(9):
            packed_ref[cell * 18 + 2 * k] = outs[k]
            packed_ref[cell * 18 + 2 * k + 1] = pltpu.roll(outs[k], 7, 0)
        count_vmem[pl.ds(cell, 1), :] = counts

    copy = pltpu.make_async_copy(count_vmem, count_ref, sem)
    copy.start()

    @pl.loop(0, columns)
    def _(column):
        value = halo_ref[(column // cells_y + 1) * ny + column % cells_y + 1]
        column_ref[column] = jnp.transpose(jnp.concatenate([value] * 16, axis=0))

    copy.wait()

    @pl.loop(0, cells)
    def _(cell):
        column = cell // 2
        begin = (cell % 2) * SLOTS
        steps = merge_cell(packed_ref, count_ref, list_ref, cell)
        blocks = (own_ref[cell] + ROWS - 1) // ROWS

        @pl.loop(0, blocks)
        def _(block):
            start = pl.multiple_of(begin + block * ROWS, ROWS)
            held = column_ref[column, pl.ds(start, ROWS), :]
            wide = (ROWS, WIDE * LANES)
            centers = [jnp.broadcast_to(held[:, 2 * c : 2 * c + 1], wide) for c in range(3)]
            slope_i = jnp.broadcast_to(held[:, 6:7], wide) if kind else None

            def step(index, sums):
                tile = jnp.concatenate([list_ref[index * WIDE + k] for k in range(WIDE)], axis=1)
                parts = pair_body(kind, centers, slope_i, tile)
                return tuple(s + fold(p) for s, p in zip(sums, parts))

            zero = jnp.zeros((ROWS, LANES), jnp.float32)
            sums = lax.fori_loop(0, steps, step, (zero,) * number)
            for k in range(number):
                sum_ref[k, column, pl.ds(start, ROWS), :] = sums[k]

    ones = jnp.ones((8, LANES), jnp.float32)
    totals = []
    for column in range(columns):
        value = halo_ref[(column // cells_y + 1) * ny + column % cells_y + 1]
        filled = value[0:1] < 0.5 * FAR
        rows = []
        for k in range(number):
            total = lax.dot_general(
                ones,
                sum_ref[k, column],
                (((1,), (1,)), ((), ())),
                precision=lax.Precision.HIGHEST,
                preferred_element_type=jnp.float32,
            )
            rows.append(jnp.where(filled, total[0:1], 0.0))
        totals.append((rows, filled))
    if kind == 0:
        density = jnp.concatenate([t[0][0] for t in totals], axis=0)
        filled = jnp.concatenate([jnp.where(t[1], 1.0, 0.0) for t in totals], axis=0)
        embed_value, embed_slope = embedding(density)
        embed_ref[...] = embed_value
        slope_ref[...] = embed_slope * filled
    else:
        filled = jnp.concatenate([jnp.where(t[1], 1.0, 0.0) for t in totals], axis=0)
        pair_sum = jnp.concatenate([t[0][0] for t in totals], axis=0)
        energy_ref[...] = filled * (embed_ref[...] + 0.5 * pair_sum)
        for c in range(3):
            force_ref[c] = jnp.concatenate([t[0][1 + c] for t in totals], axis=0)


def call_pairs(kind, dims, own, halo, embed=None):
    cells_x, cells_y = dims
    columns = cells_x * cells_y
    cells = 2 * columns
    flat = jax.ShapeDtypeStruct((columns, LANES), jnp.float32)
    vmem = pl.BlockSpec(memory_space=pltpu.VMEM)
    smem = pl.BlockSpec(memory_space=pltpu.SMEM)
    if kind == 0:
        outs, args = ((flat, flat), (own, halo))
    else:
        outs = (jax.ShapeDtypeStruct((3, columns, LANES), jnp.float32), flat)
        args = (own, halo, embed)
    number = 1 if kind == 0 else 4
    return pl.pallas_call(
        functools.partial(pair_kernel, kind, dims),
        out_shape=outs,
        in_specs=[smem] + [vmem] * (len(args) - 1),
        out_specs=(vmem, vmem),
        scratch_shapes=[
            pltpu.VMEM((cells * 18, 8, LANES), jnp.float32),
            pltpu.VMEM((cells, LANES), jnp.int32),
            pltpu.SMEM((cells, LANES), jnp.int32),
            pltpu.VMEM((18 + WIDE + 1, 8, LANES), jnp.float32),
            pltpu.VMEM((columns, LANES, LANES), jnp.float32),
            pltpu.VMEM((number, columns, LANES, LANES), jnp.float32),
            pltpu.SemaphoreType.DMA,
        ],
        compiler_params=pltpu.CompilerParams(vmem_limit_bytes=48 * 1024 * 1024),
        name="density" if kind == 0 else "forces",
    )(*args)


def swap(value, axis, dim, low, high):
    count = lax.axis_size(axis)
    up = [(i, (i + 1) % count) for i in range(count)]
    down = [(j, i) for i, j in up]
    before = lax.ppermute(high, axis, up)
    after = lax.ppermute(low, axis, down)
    return before, after


def ghosts(value):
    before, after = swap(value, "gz", 3, value[..., :SLOTS], value[..., SLOTS:])
    value = jnp.stack([value, jnp.concatenate([after, before], axis=-1)], axis=3)
    before, after = swap(value, "gx", 0, value[:1], value[-1:])
    value = jnp.concatenate([before, value, after], axis=0)
    before, after = swap(value, "gy", 1, value[:, :1], value[:, -1:])
    value = jnp.concatenate([before, value, after], axis=1)
    nx, ny, comps = value.shape[:3]
    return value.reshape(nx * ny, 2 * comps, LANES)


def on_device(positions, counts):
    cells_x, cells_y, cells_z = counts.shape
    dims = (cells_x, cells_y)
    occupied = lax.broadcasted_iota(jnp.int32, (cells_x, cells_y, cells_z, SLOTS), 3) < counts[..., None]
    occupied = occupied.reshape(1, cells_x, cells_y, cells_z * SLOTS)
    placed = jnp.where(occupied, positions, FAR)
    around = ghosts(jnp.transpose(placed, (1, 2, 0, 3)))
    own = counts.reshape(cells_x * cells_y * cells_z)
    halo = jnp.concatenate([around, jnp.zeros((around.shape[0], 2, LANES), jnp.float32)], axis=1)
    embed, slope = call_pairs(0, dims, own, halo)
    slope_around = ghosts(slope.reshape(cells_x, cells_y, 1, cells_z * SLOTS))
    halo = jnp.concatenate([around, slope_around], axis=1)
    forces, energy = call_pairs(1, dims, own, halo, embed)
    return (
        forces.reshape(3, cells_x, cells_y, cells_z * SLOTS),
        energy.reshape(cells_x, cells_y, cells_z * SLOTS),
    )


def solution(mesh):
    return jax.shard_map(
        on_device,
        mesh=mesh,
        in_specs=(P(None, "gx", "gy", "gz"), P("gx", "gy", "gz")),
        out_specs=(P(None, "gx", "gy", "gz"), P("gx", "gy", "gz")),
        check_vma=False,
    )
```

```python
import functools
import math

import jax
import jax.numpy as jnp
from jax import lax
from jax.experimental import pallas as pl
from jax.experimental.pallas import tpu as pltpu
from jax.sharding import PartitionSpec as P

SLOTS = 64
LANES = 128
FAR = 1.0e4

lattice_const = 3.615
cell_span = (2.0 * lattice_const, 2.0 * lattice_const, 4.0 * lattice_const)
cut_radius = 5.50679
cut_width = 0.50037
dens_scale = 3.80362
beta_one = 0.17394
radius_three = -2.19885
energy_one = 201.458
energy_two = 0.00659288
radius_one = 0.83591
radius_two = 4.46867
alpha_one = 2.97758
alpha_two = 1.54927
shift_delta = 0.0086225
repulsion = ((4.0, 2.24), (40.0, 1.8), (1150.0, 1.2))
embed_zero = -2.28235
embed_curve = 1.35535
lower_terms = (-1.27775, -0.86074, 1.78804, 2.97571)
upper_quartic = 0.4
upper_damping = 0.3
LOG2E = math.log2(math.e)
KEEP_SQUARED = 5.5075**2
ROWS = 16
WIDE = 2
TILES = 20


def embedding(density):
    excess = density - 1.0
    square = excess * excess
    cube = square * excess
    below_value = embed_zero + square * (
        0.5 * embed_curve
        + excess
        * (lower_terms[0] + excess * (lower_terms[1] + excess * (lower_terms[2] + excess * lower_terms[3])))
    )
    below_slope = excess * (
        embed_curve
        + excess
        * (
            3.0 * lower_terms[0]
            + excess * (4.0 * lower_terms[1] + excess * (5.0 * lower_terms[2] + excess * 6.0 * lower_terms[3]))
        )
    )
    numerator = embed_zero + square * (0.5 * embed_curve + excess * (lower_terms[0] + excess * upper_quartic))
    numer_slope = excess * (embed_curve + excess * (3.0 * lower_terms[0] + excess * 4.0 * upper_quartic))
    is_below = excess < 0.0
    denominator = jnp.where(is_below, 1.0, 1.0 + upper_damping * cube)
    above_value = numerator / denominator
    above_slope = (numer_slope - above_value * (3.0 * upper_damping) * square) / denominator
    return (
        jnp.where(is_below, below_value, above_value),
        jnp.where(is_below, below_slope, above_slope),
    )


def iota(shape, dim):
    return lax.broadcasted_iota(jnp.int32, shape, dim)


def compress_cells(halo_ref, cx, cy, ny):
    shape = (8, LANES)
    row = iota(shape, 0)
    lane = iota(shape, 1)
    comp = row // 2
    odd = row % 2
    layer = jnp.where(odd == 0, jnp.where(lane < SLOTS, 0, 1), jnp.where(lane < SLOTS, 2, -1))
    is_x, is_y, is_z = (comp == 0, comp == 1, comp == 2)
    span = jnp.where(is_z, cell_span[2], jnp.where(is_y, cell_span[1], cell_span[0]))
    counted = comp < 3
    pre = jnp.where(iota((LANES, 2 * LANES), 1) >= LANES, 1.0, 0.0)
    pre = jnp.where(iota((LANES, 2 * LANES), 0) < iota((LANES, 2 * LANES), 1), 1.0, pre).astype(jnp.bfloat16)
    data, drops = ([], [])
    for cz in (0, 1):
        add_z = jnp.where(is_z, (layer - cz).astype(jnp.float32) * cell_span[2], 0.0)
        for o1 in (-1, 0, 1):
            for o2 in (-1, 0, 1):
                add = jnp.where(is_x, o1 * cell_span[0], jnp.where(is_y, o2 * cell_span[1], add_z))
                value = halo_ref[(cx + 1 + o1) * ny + cy + 1 + o2] + add
                gap = jnp.maximum(jnp.maximum(-value, value - span), 0.0)
                gap = jnp.where(counted, gap * gap, 0.0)
                gap = gap + pltpu.roll(gap, 4, 0)
                gap = gap + pltpu.roll(gap, 2, 0)
                data.append(value)
                drops.append(gap >= KEEP_SQUARED)
    dropped = jnp.concatenate([jnp.where(d, 1.0, 0.0) for d in drops], axis=0).astype(jnp.bfloat16)
    sums = jnp.dot(dropped, pre, preferred_element_type=jnp.float32).astype(jnp.int32)
    moves = [jnp.where(drops[k], 0, sums[8 * k : 8 * k + 8, :LANES]) for k in range(18)]
    for bit in range(7):
        step = 1 << bit
        for k in range(18):
            value_in = pltpu.roll(data[k], LANES - step, 1)
            move_in = pltpu.roll(moves[k], LANES - step, 1)
            comes = (move_in & step) != 0
            data[k] = jnp.where(comes, value_in, data[k])
            moves[k] = jnp.where(comes, move_in, jnp.where((moves[k] & step) != 0, 0, moves[k]))
    counts = []
    one_row = iota((1, LANES), 1)
    for cz in (0, 1):
        line = jnp.zeros((1, LANES), jnp.int32)
        for k in range(9):
            first = 8 * (9 * cz + k)
            total = LANES - sums[first : first + 8, LANES:]
            line = jnp.where(one_row == 2 * k, total[0:1], line)
            line = jnp.where(one_row == 2 * k + 1, total[1:2], line)
        counts.append(line)
    return data, counts


def merge_cells(packed_ref, count_ref, list_ref, column):
    lane = iota((8, LANES), 1)
    offset = [jnp.int32(0), jnp.int32(0)]
    current = [jnp.zeros((8, LANES), jnp.float32) for _ in range(2)]
    for k in range(18):
        for cz in (0, 1):
            cell = column * 2 + cz
            number = count_ref[cell, k]
            place = offset[cz] & (LANES - 1)
            turned = pltpu.roll(packed_ref[cell * 18 + k], place, 1)
            current[cz] = jnp.where(lane >= place, turned, current[cz])
            list_ref[cell * TILES + (offset[cz] >> 7)] = current[cz]
            current[cz] = jnp.where(lane < place + number - LANES, turned, current[cz])
            offset[cz] = offset[cz] + number
    for cz in (0, 1):
        first = (column * 2 + cz) * TILES + (offset[cz] >> 7)
        list_ref[first] = jnp.where(lane >= (offset[cz] & (LANES - 1)), FAR, current[cz])
        for extra in range(1, WIDE):
            list_ref[first + extra] = jnp.full((8, LANES), FAR, jnp.float32)
    return offset


def pair_parts(centers, tile, slopes=None):
    d = [tile[2 * c : 2 * c + 1] - centers[c] for c in range(3)]
    squared = d[0] * d[0] + d[1] * d[1] + d[2] * d[2]
    squared = jnp.where(squared < 0.25, 100.0, squared)
    inv = lax.rsqrt(squared)
    radius = squared * inv
    scaled = jnp.minimum(radius * (1.0 / cut_width) - cut_radius / cut_width, 0.0)
    square = scaled * scaled
    quartic = square * square
    inverse = pl.reciprocal(1.0 + quartic, approx=False)
    taper = quartic * inverse
    scale = math.sqrt(beta_one * LOG2E)
    along = radius * scale - radius_three * scale
    gauss = jnp.exp2(math.log2(dens_scale) - along * along)
    if slopes is None:
        return (gauss * taper,)
    taper_slope = (square * scaled) * (inverse * inverse) * (4.0 / cut_width)
    dens_slope = gauss * (taper_slope - (along * (2.0 * beta_one / scale)) * taper)
    u = jnp.exp2(radius * (-alpha_one * LOG2E) + alpha_one * LOG2E * radius_one)
    v = jnp.exp2(radius * (-alpha_two * LOG2E) + alpha_two * LOG2E * radius_two)
    a = u * u - u
    b = v * v - v
    base = energy_one * (a - u) + (energy_two * (b - v) + shift_delta)
    base_slope = (-2.0 * alpha_one * energy_one) * a + (-2.0 * alpha_two * energy_two) * b
    pair_slope = base_slope * taper + base * taper_slope
    quarter = None
    for strength, reach in repulsion:
        close = jnp.maximum(reach - radius, 0.0)
        cubed = (4.0 * strength) * (close * close * close)
        pair_slope = pair_slope + cubed
        quarter = cubed * close if quarter is None else quarter + cubed * close
    pair_value = base * taper - 0.25 * quarter
    factor = (pair_slope + slopes * dens_slope) * inv
    return pair_value, factor * d[0], factor * d[1], factor * d[2]


def fold(value):
    total = value[:, :LANES]
    for k in range(1, WIDE):
        total = total + value[:, k * LANES : (k + 1) * LANES]
    return total


def lane_sums(value):
    high = value.astype(jnp.bfloat16)
    low = (value - high.astype(jnp.float32)).astype(jnp.bfloat16)
    both = jnp.concatenate([high, low], axis=1)
    ones = jnp.ones((8, 2 * LANES), jnp.bfloat16)
    total = lax.dot_general(ones, both, (((1,), (1,)), ((), ())), preferred_element_type=jnp.float32)
    return total[0:1]


class Exchange:
    def __init__(self, sizes, own, ref, send, recv):
        self.sizes, self.own, self.ref, self.send, self.recv = sizes, own, ref, send, recv

    def copy(self, index, source, target, axis, shift):
        count = self.sizes[axis]
        peer = lax.rem(lax.axis_index(axis) + (shift + count), count)
        return pltpu.make_async_remote_copy(
            src_ref=source,
            dst_ref=target,
            send_sem=self.send.at[index],
            recv_sem=self.recv.at[index],
            device_id={axis: peer},
            device_id_type=pl.DeviceIdType.MESH,
        )

    def phases(self):
        ref = self.ref
        cx, cy = (ref.shape[0] - 2, ref.shape[1] - 2)
        inner = ref.at[pl.ds(1, cx), pl.ds(1, cy)]
        return (
            (
                self.copy(0, self.own, inner.at[:, :, 1], "gz", 1),
                self.copy(1, self.own, inner.at[:, :, 2], "gz", -1),
            ),
            (
                self.copy(2, ref.at[pl.ds(cx, 1), pl.ds(1, cy)], ref.at[pl.ds(0, 1), pl.ds(1, cy)], "gx", 1),
                self.copy(3, ref.at[pl.ds(1, 1), pl.ds(1, cy)], ref.at[pl.ds(cx + 1, 1), pl.ds(1, cy)], "gx", -1),
            ),
            (
                self.copy(4, ref.at[:, pl.ds(cy, 1)], ref.at[:, pl.ds(0, 1)], "gy", 1),
                self.copy(5, ref.at[:, pl.ds(1, 1)], ref.at[:, pl.ds(cy + 1, 1)], "gy", -1),
            ),
        )


def run_phase(copies, wait):
    for copy in copies:
        if wait:
            copy.wait()
        else:
            copy.start()


def exchange_kernel(sizes, own_ref, *refs):
    halo_ref, around_ref, sem, send_sem, recv_sem = refs[-5:]
    cells_x, cells_y, comps = own_ref.shape[:3]
    nx, ny = (cells_x + 2, cells_y + 2)
    barrier = pltpu.get_barrier_semaphore()
    for axis, count in sizes.items():
        for shift in (1, count - 1):
            peer = lax.rem(lax.axis_index(axis) + shift, count)
            pl.semaphore_signal(
                barrier, inc=1, device_id={axis: peer}, device_id_type=pl.DeviceIdType.MESH
            )
    keep = pltpu.make_async_copy(
        own_ref, around_ref.at[pl.ds(1, cells_x), pl.ds(1, cells_y), 0], sem
    )
    keep.start()
    pl.semaphore_wait(barrier, 2 * len(sizes))
    phases = Exchange(sizes, own_ref, around_ref, send_sem, recv_sem).phases()
    run_phase(phases[0], False)
    keep.wait()
    run_phase(phases[0], True)
    for copies in phases[1:]:
        run_phase(copies, False)
        run_phase(copies, True)

    lane_row = iota((1, LANES), 1)
    low_half = lane_row < SLOTS
    lanes = lane_row.astype(jnp.float32)
    for x in range(nx):
        for y in range(ny):
            rows = []
            for c in range(comps):
                rows.append(around_ref[x, y, 0, c : c + 1])
                rows.append(
                    jnp.where(low_half, around_ref[x, y, 2, c : c + 1], around_ref[x, y, 1, c : c + 1])
                )
            rows = rows + [lanes, lanes] if comps == 3 else rows * 4
            halo_ref[x * ny + y] = jnp.concatenate(rows, axis=0)


def call_exchange(sizes, own, number, held=()):
    cells_x, cells_y, comps = own.shape[:3]
    nx, ny = (cells_x + 2, cells_y + 2)
    vmem = pl.BlockSpec(memory_space=pltpu.VMEM)
    return pl.pallas_call(
        functools.partial(exchange_kernel, sizes),
        out_shape=jax.ShapeDtypeStruct((nx * ny, 8, LANES), jnp.float32),
        in_specs=[vmem] + [pl.BlockSpec(memory_space=pl.ANY)] * len(held),
        out_specs=vmem,
        scratch_shapes=[
            pltpu.VMEM((nx, ny, 3, comps, LANES), jnp.float32),
            pltpu.SemaphoreType.DMA,
            pltpu.SemaphoreType.DMA((6,)),
            pltpu.SemaphoreType.DMA((6,)),
        ],
        compiler_params=pltpu.CompilerParams(
            vmem_limit_bytes=8 * 1024 * 1024, collective_id=number, has_side_effects=True
        ),
        name="exchange",
    )(own, *held)


def density_kernel(
    own_ref,
    placed_ref,
    halo_ref,
    slope_ref,
    embed_ref,
    packed_ref,
    list_ref,
    center_ref,
    count_vmem,
    count_ref,
    length_ref,
    sum_ref,
    sem,
):
    cells_x, cells_y = placed_ref.shape[:2]
    columns = cells_x * cells_y
    ny = cells_y + 2

    @pl.loop(0, columns)
    def _(column):
        value = placed_ref[column // cells_y, column % cells_y]
        for c in range(3):
            center_ref[column, c] = jnp.transpose(jnp.broadcast_to(value[c : c + 1], (LANES, LANES)))

    @pl.loop(0, columns)
    def _(column):
        outs, counts = compress_cells(halo_ref, column // cells_y, column % cells_y, ny)
        for k in range(18):
            packed_ref[column * 36 + 2 * k] = outs[k]
            packed_ref[column * 36 + 2 * k + 1] = pltpu.roll(outs[k], 7, 0)
        for cz in (0, 1):
            count_vmem[pl.ds(column * 2 + cz, 1), :] = counts[cz]

    copy = pltpu.make_async_copy(count_vmem, count_ref, sem)
    copy.start()
    copy.wait()

    @pl.loop(0, columns)
    def _(column):
        lengths = merge_cells(packed_ref, count_ref, list_ref, column)
        for cz in (0, 1):
            length_ref[column * 2 + cz] = (lengths[cz] + (WIDE * LANES - 1)) >> int(math.log2(WIDE * LANES))

    @pl.loop(0, 2 * columns)
    def _(cell):
        column = cell // 2
        begin = (cell % 2) * SLOTS
        steps = length_ref[cell]
        blocks = (own_ref[cell] + ROWS - 1) // ROWS

        @pl.loop(0, blocks)
        def _(block):
            start = pl.multiple_of(begin + block * ROWS, ROWS)
            centers = [
                jnp.concatenate([center_ref[column, c, pl.ds(start, ROWS), :]] * WIDE, axis=1) for c in range(3)
            ]

            def step(index, sums):
                tile = jnp.concatenate(
                    [list_ref[cell * TILES + index * WIDE + k] for k in range(WIDE)], axis=1
                )
                return (sums[0] + fold(pair_parts(centers, tile)[0]),)

            zero = jnp.zeros((ROWS, LANES), jnp.float32)
            sums = lax.fori_loop(0, steps, step, (zero,))
            sum_ref[0, column, pl.ds(start, ROWS), :] = sums[0]

    filled = jnp.concatenate(
        [placed_ref[c // cells_y, c % cells_y, 0:1] for c in range(columns)], axis=0
    ) < 0.5 * FAR
    density = jnp.concatenate([lane_sums(sum_ref[0, c]) for c in range(columns)], axis=0)
    embed_value, embed_slope = embedding(jnp.where(filled, density, 0.0))
    slope = jnp.where(filled, embed_slope, 0.0)
    for c in range(columns):
        slope_ref[c // cells_y, c % cells_y] = slope[c : c + 1]
    embed_ref[...] = embed_value


def force_kernel(
    own_ref,
    placed_ref,
    slope_own,
    embed_ref,
    halo_ref,
    packed_in,
    list_ref,
    center_ref,
    count_vmem,
    force_ref,
    energy_ref,
    packed_ref,
    slope_list,
    slope_center,
    count_ref,
    length_ref,
    sum_ref,
    sem,
):
    cells_x, cells_y = placed_ref.shape[:2]
    columns = cells_x * cells_y
    ny = cells_y + 2
    copy = pltpu.make_async_copy(count_vmem, count_ref, sem)
    copy.start()
    filled = jnp.concatenate(
        [placed_ref[c // cells_y, c % cells_y, 0:1] for c in range(columns)], axis=0
    ) < 0.5 * FAR

    @pl.loop(0, columns)
    def _(column):
        value = slope_own[column // cells_y, column % cells_y]
        slope_center[column] = jnp.transpose(jnp.broadcast_to(value, (LANES, LANES)))

    @pl.loop(0, columns)
    def _(column):
        cx, cy = (column // cells_y, column % cells_y)
        for k in range(9):
            value = halo_ref[(cx + k // 3) * ny + cy + k % 3]
            for cz in (0, 1):
                at = column * 36 + 18 * cz + 2 * k
                index = packed_in[at].astype(jnp.int32) & (LANES - 1)
                taken = jnp.take_along_axis(value, index, axis=1, mode="promise_in_bounds")
                packed_ref[at] = taken
                packed_ref[at + 1] = pltpu.roll(taken, 7, 0)

    copy.wait()

    @pl.loop(0, columns)
    def _(column):
        lengths = merge_cells(packed_ref, count_ref, slope_list, column)
        for cz in (0, 1):
            length_ref[column * 2 + cz] = (lengths[cz] + (WIDE * LANES - 1)) >> int(math.log2(WIDE * LANES))

    @pl.loop(0, 2 * columns)
    def _(cell):
        column = cell // 2
        begin = (cell % 2) * SLOTS
        steps = length_ref[cell]
        blocks = (own_ref[cell] + ROWS - 1) // ROWS

        @pl.loop(0, blocks)
        def _(block):
            start = pl.multiple_of(begin + block * ROWS, ROWS)
            centers = [
                jnp.concatenate([center_ref[column, c, pl.ds(start, ROWS), :]] * WIDE, axis=1) for c in range(3)
            ]
            slope_i = jnp.concatenate([slope_center[column, pl.ds(start, ROWS), :]] * WIDE, axis=1)

            def step(index, sums):
                at = [cell * TILES + index * WIDE + k for k in range(WIDE)]
                tile = jnp.concatenate([list_ref[t] for t in at], axis=1)
                slope_j = jnp.concatenate([slope_list[t] for t in at], axis=1)[6:7]
                parts = pair_parts(centers, tile, slope_i + slope_j)
                return tuple(total + fold(part) for total, part in zip(sums, parts))

            zero = jnp.zeros((ROWS, LANES), jnp.float32)
            sums = lax.fori_loop(0, steps, step, (zero,) * 4)
            for k in range(4):
                sum_ref[k, column, pl.ds(start, ROWS), :] = sums[k]

    pair_sum = jnp.concatenate([lane_sums(sum_ref[0, c]) for c in range(columns)], axis=0)
    energy_ref[...] = jnp.where(filled, embed_ref[...] + 0.5 * pair_sum, 0.0)
    for k in range(3):
        total = jnp.concatenate([lane_sums(sum_ref[1 + k, c]) for c in range(columns)], axis=0)
        force_ref[k] = jnp.where(filled, total, 0.0)


def on_device(positions, counts):
    cells_x, cells_y, cells_z = counts.shape
    columns = cells_x * cells_y
    cells = columns * cells_z
    occupied = lax.broadcasted_iota(jnp.int32, (cells_x, cells_y, cells_z, SLOTS), 3) < counts[..., None]
    occupied = occupied.reshape(1, cells_x, cells_y, cells_z * SLOTS)
    placed = jnp.transpose(jnp.where(occupied, positions, FAR), (1, 2, 0, 3))
    sizes = {axis: lax.axis_size(axis) for axis in ("gx", "gy", "gz")}
    own = counts.reshape(cells)
    vmem = pl.BlockSpec(memory_space=pltpu.VMEM)
    smem = pl.BlockSpec(memory_space=pltpu.SMEM)
    f32 = jnp.float32
    shape = jax.ShapeDtypeStruct
    params = pltpu.CompilerParams(vmem_limit_bytes=24 * 1024 * 1024)
    halo = call_exchange(sizes, placed, 0)
    work = [
        pltpu.SMEM((cells, LANES), jnp.int32),
        pltpu.SMEM((cells,), jnp.int32),
        pltpu.VMEM((4, columns, LANES, LANES), f32),
        pltpu.SemaphoreType.DMA,
    ]
    saved = (
        shape((cells * 18, 8, LANES), f32),
        shape((cells * TILES, 8, LANES), f32),
        shape((columns, 3, LANES, LANES), f32),
        shape((cells, LANES), jnp.int32),
    )
    slope, embed, *kept = pl.pallas_call(
        density_kernel,
        out_shape=(shape((cells_x, cells_y, 1, LANES), f32), shape((columns, LANES), f32)) + saved,
        in_specs=[smem, vmem, vmem],
        out_specs=(vmem,) * 6,
        scratch_shapes=work,
        compiler_params=params,
        name="density",
    )(own, placed, halo)
    halo = call_exchange(sizes, slope, 1)
    forces, energy = pl.pallas_call(
        force_kernel,
        out_shape=(shape((3, columns, LANES), f32), shape((columns, LANES), f32)),
        in_specs=[smem] + [vmem] * 8,
        out_specs=(vmem, vmem),
        scratch_shapes=[
            pltpu.VMEM((cells * 18, 8, LANES), f32),
            pltpu.VMEM((cells * TILES, 8, LANES), f32),
            pltpu.VMEM((columns, LANES, LANES), f32),
        ]
        + work,
        compiler_params=params,
        name="forces",
    )(own, placed, slope, embed, halo, *kept)
    return (
        forces.reshape(3, cells_x, cells_y, cells_z * SLOTS),
        energy.reshape(cells_x, cells_y, cells_z * SLOTS),
    )


def solution(mesh):
    return jax.shard_map(
        on_device,
        mesh=mesh,
        in_specs=(P(None, "gx", "gy", "gz"), P("gx", "gy", "gz")),
        out_specs=(P(None, "gx", "gy", "gz"), P("gx", "gy", "gz")),
        check_vma=False,
    )
```

```python
import functools
import math

import jax
import jax.numpy as jnp
from jax import lax
from jax.experimental import pallas as pl
from jax.experimental.pallas import tpu as pltpu
from jax.sharding import PartitionSpec as P

SLOTS = 64
LANES = 128
FAR = 1.0e4

lattice_const = 3.615
cell_span = (2.0 * lattice_const, 2.0 * lattice_const, 4.0 * lattice_const)
cut_radius = 5.50679
cut_width = 0.50037
dens_scale = 3.80362
beta_one = 0.17394
radius_three = -2.19885
energy_one = 201.458
energy_two = 0.00659288
radius_one = 0.83591
radius_two = 4.46867
alpha_one = 2.97758
alpha_two = 1.54927
shift_delta = 0.0086225
repulsion = ((4.0, 2.24), (40.0, 1.8), (1150.0, 1.2))
embed_zero = -2.28235
embed_curve = 1.35535
lower_terms = (-1.27775, -0.86074, 1.78804, 2.97571)
upper_quartic = 0.4
upper_damping = 0.3
LOG2E = math.log2(math.e)
KEEP_SQUARED = 5.5075**2
ROWS = 16
WIDE = 2
TILES = 20


def embedding(density):
    excess = density - 1.0
    square = excess * excess
    cube = square * excess
    below_value = embed_zero + square * (
        0.5 * embed_curve
        + excess
        * (lower_terms[0] + excess * (lower_terms[1] + excess * (lower_terms[2] + excess * lower_terms[3])))
    )
    below_slope = excess * (
        embed_curve
        + excess
        * (
            3.0 * lower_terms[0]
            + excess * (4.0 * lower_terms[1] + excess * (5.0 * lower_terms[2] + excess * 6.0 * lower_terms[3]))
        )
    )
    numerator = embed_zero + square * (0.5 * embed_curve + excess * (lower_terms[0] + excess * upper_quartic))
    numer_slope = excess * (embed_curve + excess * (3.0 * lower_terms[0] + excess * 4.0 * upper_quartic))
    is_below = excess < 0.0
    denominator = jnp.where(is_below, 1.0, 1.0 + upper_damping * cube)
    above_value = numerator / denominator
    above_slope = (numer_slope - above_value * (3.0 * upper_damping) * square) / denominator
    return (
        jnp.where(is_below, below_value, above_value),
        jnp.where(is_below, below_slope, above_slope),
    )


def iota(shape, dim):
    return lax.broadcasted_iota(jnp.int32, shape, dim)


def compress_cells(halo_ref, cx, cy, ny):
    shape = (8, LANES)
    row = iota(shape, 0)
    lane = iota(shape, 1)
    comp = row // 2
    odd = row % 2
    layer = jnp.where(odd == 0, jnp.where(lane < SLOTS, 0, 1), jnp.where(lane < SLOTS, 2, -1))
    is_x, is_y, is_z = (comp == 0, comp == 1, comp == 2)
    span = jnp.where(is_z, cell_span[2], jnp.where(is_y, cell_span[1], cell_span[0]))
    counted = comp < 3
    pre = jnp.where(iota((LANES, 2 * LANES), 1) >= LANES, 1.0, 0.0)
    pre = jnp.where(iota((LANES, 2 * LANES), 0) < iota((LANES, 2 * LANES), 1), 1.0, pre).astype(jnp.bfloat16)
    data, drops = ([], [])
    for cz in (0, 1):
        add_z = jnp.where(is_z, (layer - cz).astype(jnp.float32) * cell_span[2], 0.0)
        for o1 in (-1, 0, 1):
            for o2 in (-1, 0, 1):
                add = jnp.where(is_x, o1 * cell_span[0], jnp.where(is_y, o2 * cell_span[1], add_z))
                value = halo_ref[(cx + 1 + o1) * ny + cy + 1 + o2] + add
                gap = jnp.maximum(jnp.maximum(-value, value - span), 0.0)
                gap = jnp.where(counted, gap * gap, 0.0)
                gap = gap + pltpu.roll(gap, 4, 0)
                gap = gap + pltpu.roll(gap, 2, 0)
                data.append(value)
                drops.append(gap >= KEEP_SQUARED)
    dropped = [jnp.where(d, 1.0, 0.0) for d in drops]
    groups = []
    for first in range(0, 18, 4):
        merged = dropped[first]
        for k in range(first + 1, min(first + 4, 18)):
            merged = jnp.where(comp == k - first, dropped[k], merged)
        groups.append(merged)
    sums = jnp.dot(
        jnp.concatenate(groups, axis=0).astype(jnp.bfloat16), pre, preferred_element_type=jnp.float32
    ).astype(jnp.int32)
    moves = [
        jnp.where(g > 0.5, 0, sums[8 * n : 8 * n + 8, :LANES]) for n, g in enumerate(groups)
    ]
    for bit in range(7):
        step = 1 << bit
        for n in range(len(moves)):
            move_in = pltpu.roll(moves[n], LANES - step, 1)
            stay = jnp.where((moves[n] & step) != 0, 0, moves[n])
            moves[n] = jnp.where((move_in & step) != 0, move_in, stay)
    indices = [lane + move for move in moves]
    for k in range(18):
        index = jnp.where(comp == k % 4, indices[k // 4], 0)
        index = index + pltpu.roll(index, 4, 0)
        index = index + pltpu.roll(index, 2, 0)
        data[k] = jnp.take_along_axis(data[k], index & (LANES - 1), axis=1, mode="promise_in_bounds")
    counts = []
    one_row = iota((1, LANES), 1)
    for cz in (0, 1):
        line = jnp.zeros((1, LANES), jnp.int32)
        for k in range(9):
            first = 2 * (9 * cz + k)
            total = LANES - sums[first : first + 2, LANES:]
            line = jnp.where(one_row == 2 * k, total[0:1], line)
            line = jnp.where(one_row == 2 * k + 1, total[1:2], line)
        counts.append(line)
    return data, counts


def merge_cells(packed_ref, count_ref, list_ref, column):
    lane = iota((8, LANES), 1)
    offset = [jnp.int32(0), jnp.int32(0)]
    current = [jnp.zeros((8, LANES), jnp.float32) for _ in range(2)]
    for k in range(18):
        for cz in (0, 1):
            cell = column * 2 + cz
            number = count_ref[cell, k]
            place = offset[cz] & (LANES - 1)
            turned = pltpu.roll(packed_ref[cell * 18 + k], place, 1)
            current[cz] = jnp.where(lane >= place, turned, current[cz])
            list_ref[cell * TILES + (offset[cz] >> 7)] = current[cz]
            current[cz] = jnp.where(lane < place + number - LANES, turned, current[cz])
            offset[cz] = offset[cz] + number
    for cz in (0, 1):
        first = (column * 2 + cz) * TILES + (offset[cz] >> 7)
        list_ref[first] = jnp.where(lane >= (offset[cz] & (LANES - 1)), FAR, current[cz])
        for extra in range(1, WIDE):
            list_ref[first + extra] = jnp.full((8, LANES), FAR, jnp.float32)
    return offset


def pair_parts(centers, tile, slopes=None):
    d = [tile[2 * c : 2 * c + 1] - centers[c] for c in range(3)]
    squared = d[0] * d[0] + d[1] * d[1] + d[2] * d[2]
    squared = jnp.where(squared < 0.25, 100.0, squared)
    inv = lax.rsqrt(squared)
    radius = squared * inv
    scaled = jnp.minimum(radius * (1.0 / cut_width) - cut_radius / cut_width, 0.0)
    square = scaled * scaled
    quartic = square * square
    bottom = 1.0 + quartic
    inverse = pl.reciprocal(bottom, approx=True)
    inverse = inverse * (2.0 - bottom * inverse)
    taper = quartic * inverse
    scale = math.sqrt(beta_one * LOG2E)
    along = radius * scale - radius_three * scale
    gauss = jnp.exp2(math.log2(dens_scale) - along * along)
    if slopes is None:
        return (gauss * taper,)
    taper_slope = (square * scaled) * (inverse * inverse) * (4.0 / cut_width)
    dens_slope = gauss * (taper_slope - (along * (2.0 * beta_one / scale)) * taper)
    u = jnp.exp2(radius * (-alpha_one * LOG2E) + alpha_one * LOG2E * radius_one)
    v = jnp.exp2(radius * (-alpha_two * LOG2E) + alpha_two * LOG2E * radius_two)
    a = u * u - u
    b = v * v - v
    base = energy_one * (a - u) + (energy_two * (b - v) + shift_delta)
    base_slope = (-2.0 * alpha_one * energy_one) * a + (-2.0 * alpha_two * energy_two) * b
    pair_slope = base_slope * taper + base * taper_slope
    quarter = None
    for strength, reach in repulsion:
        close = jnp.maximum(reach - radius, 0.0)
        cubed = (4.0 * strength) * (close * close * close)
        pair_slope = pair_slope + cubed
        quarter = cubed * close if quarter is None else quarter + cubed * close
    pair_value = base * taper - 0.25 * quarter
    factor = (pair_slope + slopes * dens_slope) * inv
    return pair_value, factor * d[0], factor * d[1], factor * d[2]


def fold(value):
    total = value[:, :LANES]
    for k in range(1, WIDE):
        total = total + value[:, k * LANES : (k + 1) * LANES]
    return total


def lane_sums(value):
    high = value.astype(jnp.bfloat16)
    low = (value - high.astype(jnp.float32)).astype(jnp.bfloat16)
    both = jnp.concatenate([high, low], axis=1)
    ones = jnp.ones((8, 2 * LANES), jnp.bfloat16)
    total = lax.dot_general(ones, both, (((1,), (1,)), ((), ())), preferred_element_type=jnp.float32)
    return total[0:1]


def edge(shift, cells):
    if shift == 0:
        return pl.ds(0, cells), pl.ds(1, cells)
    if shift > 0:
        return pl.ds(cells - 1, 1), pl.ds(0, 1)
    return pl.ds(0, 1), pl.ds(cells + 1, 1)


def exchange_kernel(sizes, own_ref, *refs):
    halo_ref, around_ref, sem, send_sem, recv_sem = refs[-5:]
    cells_x, cells_y, comps = own_ref.shape[:3]
    nx, ny = (cells_x + 2, cells_y + 2)
    shifts = [
        (x, y, z) for x in (0, 1, -1) for y in (0, 1, -1) for z in (0, 1, -1) if (x, y, z) != (0, 0, 0)
    ]
    peers = [
        {axis: lax.rem(lax.axis_index(axis) + (step + sizes[axis]), sizes[axis]) for axis, step in zip(sizes, shift)}
        for shift in shifts
    ]
    barrier = pltpu.get_barrier_semaphore()
    for peer in peers:
        pl.semaphore_signal(barrier, inc=1, device_id=peer, device_id_type=pl.DeviceIdType.MESH)
    keep = pltpu.make_async_copy(own_ref, around_ref.at[pl.ds(1, cells_x), pl.ds(1, cells_y), 0], sem)
    keep.start()
    pl.semaphore_wait(barrier, len(shifts))
    copies = []
    for index, (shift, peer) in enumerate(zip(shifts, peers)):
        from_x, to_x = edge(shift[0], cells_x)
        from_y, to_y = edge(shift[1], cells_y)
        copies.append(
            pltpu.make_async_remote_copy(
                src_ref=own_ref.at[from_x, from_y],
                dst_ref=around_ref.at[to_x, to_y, shift[2] % 3],
                send_sem=send_sem.at[index],
                recv_sem=recv_sem.at[index],
                device_id=peer,
                device_id_type=pl.DeviceIdType.MESH,
            )
        )
        copies[-1].start()
    keep.wait()
    for copy in copies:
        copy.wait()

    lane_row = iota((1, LANES), 1)
    low_half = lane_row < SLOTS
    lanes = lane_row.astype(jnp.float32)
    for x in range(nx):
        for y in range(ny):
            rows = []
            for c in range(comps):
                rows.append(around_ref[x, y, 0, c : c + 1])
                rows.append(
                    jnp.where(low_half, around_ref[x, y, 2, c : c + 1], around_ref[x, y, 1, c : c + 1])
                )
            rows = rows + [lanes, lanes] if comps == 3 else rows * 4
            halo_ref[x * ny + y] = jnp.concatenate(rows, axis=0)


def call_exchange(sizes, own, number, held=()):
    cells_x, cells_y, comps = own.shape[:3]
    nx, ny = (cells_x + 2, cells_y + 2)
    vmem = pl.BlockSpec(memory_space=pltpu.VMEM)
    return pl.pallas_call(
        functools.partial(exchange_kernel, sizes),
        out_shape=jax.ShapeDtypeStruct((nx * ny, 8, LANES), jnp.float32),
        in_specs=[vmem] + [pl.BlockSpec(memory_space=pl.ANY)] * len(held),
        out_specs=vmem,
        scratch_shapes=[
            pltpu.VMEM((nx, ny, 3, comps, LANES), jnp.float32),
            pltpu.SemaphoreType.DMA,
            pltpu.SemaphoreType.DMA((26,)),
            pltpu.SemaphoreType.DMA((26,)),
        ],
        compiler_params=pltpu.CompilerParams(
            vmem_limit_bytes=8 * 1024 * 1024, collective_id=number, has_side_effects=True
        ),
        name="exchange",
    )(own, *held)


def density_kernel(
    own_ref,
    placed_ref,
    halo_ref,
    slope_ref,
    embed_ref,
    packed_ref,
    list_ref,
    center_ref,
    count_vmem,
    count_ref,
    length_ref,
    sum_ref,
    sem,
):
    cells_x, cells_y = placed_ref.shape[:2]
    columns = cells_x * cells_y
    ny = cells_y + 2

    @pl.loop(0, columns)
    def _(column):
        value = placed_ref[column // cells_y, column % cells_y]
        for c in range(3):
            center_ref[column, c] = jnp.transpose(jnp.broadcast_to(value[c : c + 1], (LANES, LANES)))

    @pl.loop(0, columns)
    def _(column):
        outs, counts = compress_cells(halo_ref, column // cells_y, column % cells_y, ny)
        for k in range(18):
            packed_ref[column * 36 + 2 * k] = outs[k]
            packed_ref[column * 36 + 2 * k + 1] = pltpu.roll(outs[k], 7, 0)
        for cz in (0, 1):
            count_vmem[pl.ds(column * 2 + cz, 1), :] = counts[cz]

    copy = pltpu.make_async_copy(count_vmem, count_ref, sem)
    copy.start()
    copy.wait()

    @pl.loop(0, columns)
    def _(column):
        lengths = merge_cells(packed_ref, count_ref, list_ref, column)
        for cz in (0, 1):
            length_ref[column * 2 + cz] = (lengths[cz] + (WIDE * LANES - 1)) >> int(math.log2(WIDE * LANES))

    @pl.loop(0, 2 * columns)
    def _(cell):
        column = cell // 2
        begin = (cell % 2) * SLOTS
        steps = length_ref[cell]
        blocks = (own_ref[cell] + ROWS - 1) // ROWS

        @pl.loop(0, blocks)
        def _(block):
            start = pl.multiple_of(begin + block * ROWS, ROWS)
            centers = [
                jnp.concatenate([center_ref[column, c, pl.ds(start, ROWS), :]] * WIDE, axis=1) for c in range(3)
            ]

            def step(index, sums):
                tile = jnp.concatenate(
                    [list_ref[cell * TILES + index * WIDE + k] for k in range(WIDE)], axis=1
                )
                return (sums[0] + fold(pair_parts(centers, tile)[0]),)

            zero = jnp.zeros((ROWS, LANES), jnp.float32)
            sums = lax.fori_loop(0, steps, step, (zero,))
            sum_ref[0, column, pl.ds(start, ROWS), :] = sums[0]

    filled = jnp.concatenate(
        [placed_ref[c // cells_y, c % cells_y, 0:1] for c in range(columns)], axis=0
    ) < 0.5 * FAR
    density = jnp.concatenate([lane_sums(sum_ref[0, c]) for c in range(columns)], axis=0)
    embed_value, embed_slope = embedding(jnp.where(filled, density, 0.0))
    slope = jnp.where(filled, embed_slope, 0.0)
    for c in range(columns):
        slope_ref[c // cells_y, c % cells_y] = slope[c : c + 1]
    embed_ref[...] = embed_value


def force_kernel(
    own_ref,
    placed_ref,
    slope_own,
    embed_ref,
    halo_ref,
    packed_in,
    list_ref,
    center_ref,
    count_vmem,
    force_ref,
    energy_ref,
    packed_ref,
    slope_list,
    slope_center,
    count_ref,
    length_ref,
    sum_ref,
    sem,
):
    cells_x, cells_y = placed_ref.shape[:2]
    columns = cells_x * cells_y
    ny = cells_y + 2
    copy = pltpu.make_async_copy(count_vmem, count_ref, sem)
    copy.start()
    filled = jnp.concatenate(
        [placed_ref[c // cells_y, c % cells_y, 0:1] for c in range(columns)], axis=0
    ) < 0.5 * FAR

    @pl.loop(0, columns)
    def _(column):
        value = slope_own[column // cells_y, column % cells_y]
        slope_center[column] = jnp.transpose(jnp.broadcast_to(value, (LANES, LANES)))

    @pl.loop(0, columns)
    def _(column):
        cx, cy = (column // cells_y, column % cells_y)
        for k in range(9):
            value = halo_ref[(cx + k // 3) * ny + cy + k % 3]
            for cz in (0, 1):
                at = column * 36 + 18 * cz + 2 * k
                index = packed_in[at].astype(jnp.int32) & (LANES - 1)
                taken = jnp.take_along_axis(value, index, axis=1, mode="promise_in_bounds")
                packed_ref[at] = taken
                packed_ref[at + 1] = pltpu.roll(taken, 7, 0)

    copy.wait()

    @pl.loop(0, columns)
    def _(column):
        lengths = merge_cells(packed_ref, count_ref, slope_list, column)
        for cz in (0, 1):
            length_ref[column * 2 + cz] = (lengths[cz] + (WIDE * LANES - 1)) >> int(math.log2(WIDE * LANES))

    @pl.loop(0, 2 * columns)
    def _(cell):
        column = cell // 2
        begin = (cell % 2) * SLOTS
        steps = length_ref[cell]
        blocks = (own_ref[cell] + ROWS - 1) // ROWS

        @pl.loop(0, blocks)
        def _(block):
            start = pl.multiple_of(begin + block * ROWS, ROWS)
            centers = [
                jnp.concatenate([center_ref[column, c, pl.ds(start, ROWS), :]] * WIDE, axis=1) for c in range(3)
            ]
            slope_i = jnp.concatenate([slope_center[column, pl.ds(start, ROWS), :]] * WIDE, axis=1)

            def step(index, sums):
                at = [cell * TILES + index * WIDE + k for k in range(WIDE)]
                tile = jnp.concatenate([list_ref[t] for t in at], axis=1)
                slope_j = jnp.concatenate([slope_list[t] for t in at], axis=1)[6:7]
                parts = pair_parts(centers, tile, slope_i + slope_j)
                return tuple(total + fold(part) for total, part in zip(sums, parts))

            zero = jnp.zeros((ROWS, LANES), jnp.float32)
            sums = lax.fori_loop(0, steps, step, (zero,) * 4)
            for k in range(4):
                sum_ref[k, column, pl.ds(start, ROWS), :] = sums[k]

    pair_sum = jnp.concatenate([lane_sums(sum_ref[0, c]) for c in range(columns)], axis=0)
    energy_ref[...] = jnp.where(filled, embed_ref[...] + 0.5 * pair_sum, 0.0)
    for k in range(3):
        total = jnp.concatenate([lane_sums(sum_ref[1 + k, c]) for c in range(columns)], axis=0)
        force_ref[k] = jnp.where(filled, total, 0.0)


def on_device(positions, counts):
    cells_x, cells_y, cells_z = counts.shape
    columns = cells_x * cells_y
    cells = columns * cells_z
    occupied = lax.broadcasted_iota(jnp.int32, (cells_x, cells_y, cells_z, SLOTS), 3) < counts[..., None]
    occupied = occupied.reshape(1, cells_x, cells_y, cells_z * SLOTS)
    placed = jnp.transpose(jnp.where(occupied, positions, FAR), (1, 2, 0, 3))
    sizes = {axis: lax.axis_size(axis) for axis in ("gx", "gy", "gz")}
    own = counts.reshape(cells)
    vmem = pl.BlockSpec(memory_space=pltpu.VMEM)
    smem = pl.BlockSpec(memory_space=pltpu.SMEM)
    f32 = jnp.float32
    shape = jax.ShapeDtypeStruct
    params = pltpu.CompilerParams(vmem_limit_bytes=24 * 1024 * 1024)
    halo = call_exchange(sizes, placed, 0)
    work = [
        pltpu.SMEM((cells, LANES), jnp.int32),
        pltpu.SMEM((cells,), jnp.int32),
        pltpu.VMEM((4, columns, LANES, LANES), f32),
        pltpu.SemaphoreType.DMA,
    ]
    saved = (
        shape((cells * 18, 8, LANES), f32),
        shape((cells * TILES, 8, LANES), f32),
        shape((columns, 3, LANES, LANES), f32),
        shape((cells, LANES), jnp.int32),
    )
    slope, embed, *kept = pl.pallas_call(
        density_kernel,
        out_shape=(shape((cells_x, cells_y, 1, LANES), f32), shape((columns, LANES), f32)) + saved,
        in_specs=[smem, vmem, vmem],
        out_specs=(vmem,) * 6,
        scratch_shapes=work,
        compiler_params=params,
        name="density",
    )(own, placed, halo)
    halo = call_exchange(sizes, slope, 1)
    forces, energy = pl.pallas_call(
        force_kernel,
        out_shape=(shape((3, columns, LANES), f32), shape((columns, LANES), f32)),
        in_specs=[smem] + [vmem] * 8,
        out_specs=(vmem, vmem),
        scratch_shapes=[
            pltpu.VMEM((cells * 18, 8, LANES), f32),
            pltpu.VMEM((cells * TILES, 8, LANES), f32),
            pltpu.VMEM((columns, LANES, LANES), f32),
        ]
        + work,
        compiler_params=params,
        name="forces",
    )(own, placed, slope, embed, halo, *kept)
    return (
        forces.reshape(3, cells_x, cells_y, cells_z * SLOTS),
        energy.reshape(cells_x, cells_y, cells_z * SLOTS),
    )


def solution(mesh):
    return jax.shard_map(
        on_device,
        mesh=mesh,
        in_specs=(P(None, "gx", "gy", "gz"), P("gx", "gy", "gz")),
        out_specs=(P(None, "gx", "gy", "gz"), P("gx", "gy", "gz")),
        check_vma=False,
    )
```

```python
import functools
import math

import jax
import jax.numpy as jnp
from jax import lax
from jax.experimental import pallas as pl
from jax.experimental.pallas import tpu as pltpu
from jax.sharding import PartitionSpec as P

SLOTS = 64
LANES = 128
FAR = 1.0e4

lattice_const = 3.615
cell_span = (2.0 * lattice_const, 2.0 * lattice_const, 4.0 * lattice_const)
cut_radius = 5.50679
cut_width = 0.50037
dens_scale = 3.80362
beta_one = 0.17394
radius_three = -2.19885
energy_one = 201.458
energy_two = 0.00659288
radius_one = 0.83591
radius_two = 4.46867
alpha_one = 2.97758
alpha_two = 1.54927
shift_delta = 0.0086225
repulsion = ((4.0, 2.24), (40.0, 1.8), (1150.0, 1.2))
embed_zero = -2.28235
embed_curve = 1.35535
lower_terms = (-1.27775, -0.86074, 1.78804, 2.97571)
upper_quartic = 0.4
upper_damping = 0.3
LOG2E = math.log2(math.e)
KEEP_SQUARED = 5.5075**2
ROWS = 16
DENSE_ROWS = 32
WIDE = 2
TILES = 20


def embedding(density):
    excess = density - 1.0
    square = excess * excess
    cube = square * excess
    below_value = embed_zero + square * (
        0.5 * embed_curve
        + excess
        * (lower_terms[0] + excess * (lower_terms[1] + excess * (lower_terms[2] + excess * lower_terms[3])))
    )
    below_slope = excess * (
        embed_curve
        + excess
        * (
            3.0 * lower_terms[0]
            + excess * (4.0 * lower_terms[1] + excess * (5.0 * lower_terms[2] + excess * 6.0 * lower_terms[3]))
        )
    )
    numerator = embed_zero + square * (0.5 * embed_curve + excess * (lower_terms[0] + excess * upper_quartic))
    numer_slope = excess * (embed_curve + excess * (3.0 * lower_terms[0] + excess * 4.0 * upper_quartic))
    is_below = excess < 0.0
    denominator = jnp.where(is_below, 1.0, 1.0 + upper_damping * cube)
    above_value = numerator / denominator
    above_slope = (numer_slope - above_value * (3.0 * upper_damping) * square) / denominator
    return (
        jnp.where(is_below, below_value, above_value),
        jnp.where(is_below, below_slope, above_slope),
    )


def iota(shape, dim):
    return lax.broadcasted_iota(jnp.int32, shape, dim)


def compress_cells(halo_ref, cx, cy, ny):
    shape = (8, LANES)
    row = iota(shape, 0)
    lane = iota(shape, 1)
    comp = row // 2
    odd = row % 2
    layer = jnp.where(odd == 0, jnp.where(lane < SLOTS, 0, 1), jnp.where(lane < SLOTS, 2, -1))
    is_x, is_y, is_z = (comp == 0, comp == 1, comp == 2)
    span = jnp.where(is_z, cell_span[2], jnp.where(is_y, cell_span[1], cell_span[0]))
    counted = comp < 3
    pre = jnp.where(iota((LANES, 2 * LANES), 1) >= LANES, 1.0, 0.0)
    pre = jnp.where(iota((LANES, 2 * LANES), 0) < iota((LANES, 2 * LANES), 1), 1.0, pre).astype(jnp.bfloat16)
    data, drops = ([], [])
    for cz in (0, 1):
        add_z = jnp.where(is_z, (layer - cz).astype(jnp.float32) * cell_span[2], 0.0)
        for o1 in (-1, 0, 1):
            for o2 in (-1, 0, 1):
                add = jnp.where(is_x, o1 * cell_span[0], jnp.where(is_y, o2 * cell_span[1], add_z))
                value = halo_ref[(cx + 1 + o1) * ny + cy + 1 + o2] + add
                gap = jnp.maximum(jnp.maximum(-value, value - span), 0.0)
                gap = jnp.where(counted, gap * gap, 0.0)
                gap = gap + pltpu.roll(gap, 4, 0)
                gap = gap + pltpu.roll(gap, 2, 0)
                data.append(value)
                drops.append(gap >= KEEP_SQUARED)
    dropped = jnp.concatenate([jnp.where(d, 1.0, 0.0) for d in drops], axis=0).astype(jnp.bfloat16)
    sums = jnp.dot(dropped, pre, preferred_element_type=jnp.float32).astype(jnp.int32)
    moves = [jnp.where(drops[k], 0, sums[8 * k : 8 * k + 8, :LANES]) for k in range(18)]
    for bit in range(7):
        step = 1 << bit
        for k in range(18):
            value_in = pltpu.roll(data[k], LANES - step, 1)
            move_in = pltpu.roll(moves[k], LANES - step, 1)
            comes = (move_in & step) != 0
            data[k] = jnp.where(comes, value_in, data[k])
            moves[k] = jnp.where(comes, move_in, jnp.where((moves[k] & step) != 0, 0, moves[k]))
    counts = []
    one_row = iota((1, LANES), 1)
    for cz in (0, 1):
        line = jnp.zeros((1, LANES), jnp.int32)
        for k in range(9):
            first = 8 * (9 * cz + k)
            total = LANES - sums[first : first + 8, LANES:]
            line = jnp.where(one_row == 2 * k, total[0:1], line)
            line = jnp.where(one_row == 2 * k + 1, total[1:2], line)
        counts.append(line)
    return data, counts


def merge_cells(packed_ref, count_ref, list_ref, column):
    lane = iota((8, LANES), 1)
    offset = [jnp.int32(0), jnp.int32(0)]
    current = [jnp.zeros((8, LANES), jnp.float32) for _ in range(2)]
    for k in range(18):
        for cz in (0, 1):
            cell = column * 2 + cz
            number = count_ref[cell, k]
            place = offset[cz] & (LANES - 1)
            turned = pltpu.roll(packed_ref[cell * 18 + k], place, 1)
            current[cz] = jnp.where(lane >= place, turned, current[cz])
            list_ref[cell * TILES + (offset[cz] >> 7)] = current[cz]
            current[cz] = jnp.where(lane < place + number - LANES, turned, current[cz])
            offset[cz] = offset[cz] + number
    for cz in (0, 1):
        first = (column * 2 + cz) * TILES + (offset[cz] >> 7)
        list_ref[first] = jnp.where(lane >= (offset[cz] & (LANES - 1)), FAR, current[cz])
        for extra in range(1, WIDE):
            list_ref[first + extra] = jnp.full((8, LANES), FAR, jnp.float32)
    return offset


def pair_parts(centers, tile, slopes=None):
    d = [tile[2 * c : 2 * c + 1] - centers[c] for c in range(3)]
    squared = d[0] * d[0] + d[1] * d[1] + d[2] * d[2]
    squared = jnp.where(squared < 0.25, 100.0, squared)
    inv = lax.rsqrt(squared)
    radius = squared * inv
    scaled = jnp.minimum(radius * (1.0 / cut_width) - cut_radius / cut_width, 0.0)
    square = scaled * scaled
    quartic = square * square
    inverse = pl.reciprocal(1.0 + quartic, approx=False)
    taper = quartic * inverse
    scale = math.sqrt(beta_one * LOG2E)
    along = radius * scale - radius_three * scale
    gauss = jnp.exp2(math.log2(dens_scale) - along * along)
    if slopes is None:
        return (gauss * taper,)
    taper_slope = (square * scaled) * (inverse * inverse) * (4.0 / cut_width)
    dens_slope = gauss * (taper_slope - (along * (2.0 * beta_one / scale)) * taper)
    u = jnp.exp2(radius * (-alpha_one * LOG2E) + alpha_one * LOG2E * radius_one)
    v = jnp.exp2(radius * (-alpha_two * LOG2E) + alpha_two * LOG2E * radius_two)
    a = u * u - u
    b = v * v - v
    base = energy_one * (a - u) + (energy_two * (b - v) + shift_delta)
    base_slope = (-2.0 * alpha_one * energy_one) * a + (-2.0 * alpha_two * energy_two) * b
    pair_slope = base_slope * taper + base * taper_slope
    quarter = None
    for strength, reach in repulsion:
        close = jnp.maximum(reach - radius, 0.0)
        cubed = (4.0 * strength) * (close * close * close)
        pair_slope = pair_slope + cubed
        quarter = cubed * close if quarter is None else quarter + cubed * close
    pair_value = base * taper - 0.25 * quarter
    factor = (pair_slope + slopes * dens_slope) * inv
    return pair_value, factor * d[0], factor * d[1], factor * d[2]


def fold(value):
    total = value[:, :LANES]
    for k in range(1, WIDE):
        total = total + value[:, k * LANES : (k + 1) * LANES]
    return total


def lane_sums(value):
    high = value.astype(jnp.bfloat16)
    low = (value - high.astype(jnp.float32)).astype(jnp.bfloat16)
    both = jnp.concatenate([high, low], axis=1)
    ones = jnp.ones((8, 2 * LANES), jnp.bfloat16)
    total = lax.dot_general(ones, both, (((1,), (1,)), ((), ())), preferred_element_type=jnp.float32)
    return total[0:1]


def edge(shift, cells):
    if shift == 0:
        return pl.ds(0, cells), pl.ds(1, cells)
    if shift > 0:
        return pl.ds(cells - 1, 1), pl.ds(0, 1)
    return pl.ds(0, 1), pl.ds(cells + 1, 1)


def exchange_kernel(sizes, own_ref, halo_ref, center_ref, around_ref, sem, send_sem, recv_sem):
    cells_x, cells_y, comps = own_ref.shape[:3]
    nx, ny = (cells_x + 2, cells_y + 2)
    shifts = [
        (x, y, z) for x in (0, 1, -1) for y in (0, 1, -1) for z in (0, 1, -1) if (x, y, z) != (0, 0, 0)
    ]
    peers = [
        {axis: lax.rem(lax.axis_index(axis) + (step + sizes[axis]), sizes[axis]) for axis, step in zip(sizes, shift)}
        for shift in shifts
    ]
    barrier = pltpu.get_barrier_semaphore()
    for peer in peers:
        pl.semaphore_signal(barrier, inc=1, device_id=peer, device_id_type=pl.DeviceIdType.MESH)
    keep = pltpu.make_async_copy(own_ref, around_ref.at[pl.ds(1, cells_x), pl.ds(1, cells_y), 0], sem)
    keep.start()
    pl.semaphore_wait(barrier, len(shifts))
    copies = []
    for index, (shift, peer) in enumerate(zip(shifts, peers)):
        from_x, to_x = edge(shift[0], cells_x)
        from_y, to_y = edge(shift[1], cells_y)
        copies.append(
            pltpu.make_async_remote_copy(
                src_ref=own_ref.at[from_x, from_y],
                dst_ref=around_ref.at[to_x, to_y, shift[2] % 3],
                send_sem=send_sem.at[index],
                recv_sem=recv_sem.at[index],
                device_id=peer,
                device_id_type=pl.DeviceIdType.MESH,
            )
        )
        copies[-1].start()

    @pl.loop(0, cells_x)
    def _(x):
        for y in range(cells_y):
            value = own_ref[x, y]
            for c in range(comps):
                center_ref[x * cells_y + y, c] = jnp.transpose(
                    jnp.broadcast_to(value[c : c + 1], (LANES, LANES))
                )

    keep.wait()
    for copy in copies:
        copy.wait()

    lane_row = iota((1, LANES), 1)
    low_half = lane_row < SLOTS
    lanes = lane_row.astype(jnp.float32)
    for x in range(nx):
        for y in range(ny):
            rows = []
            for c in range(comps):
                rows.append(around_ref[x, y, 0, c : c + 1])
                rows.append(
                    jnp.where(low_half, around_ref[x, y, 2, c : c + 1], around_ref[x, y, 1, c : c + 1])
                )
            rows = rows + [lanes, lanes] if comps == 3 else rows * 4
            halo_ref[x * ny + y] = jnp.concatenate(rows, axis=0)


def call_exchange(sizes, own, number):
    cells_x, cells_y, comps = own.shape[:3]
    nx, ny = (cells_x + 2, cells_y + 2)
    vmem = pl.BlockSpec(memory_space=pltpu.VMEM)
    return pl.pallas_call(
        functools.partial(exchange_kernel, sizes),
        out_shape=(
            jax.ShapeDtypeStruct((nx * ny, 8, LANES), jnp.float32),
            jax.ShapeDtypeStruct((cells_x * cells_y, comps, LANES, LANES), jnp.float32),
        ),
        in_specs=[vmem],
        out_specs=(vmem, vmem),
        scratch_shapes=[
            pltpu.VMEM((nx, ny, 3, comps, LANES), jnp.float32),
            pltpu.SemaphoreType.DMA,
            pltpu.SemaphoreType.DMA((26,)),
            pltpu.SemaphoreType.DMA((26,)),
        ],
        compiler_params=pltpu.CompilerParams(
            vmem_limit_bytes=8 * 1024 * 1024, collective_id=number, has_side_effects=True
        ),
        name="exchange",
    )(own)


def density_kernel(
    own_ref,
    placed_ref,
    halo_ref,
    center_ref,
    slope_ref,
    embed_ref,
    packed_ref,
    list_ref,
    count_vmem,
    count_ref,
    length_ref,
    sum_ref,
    sem,
):
    cells_x, cells_y = placed_ref.shape[:2]
    columns = cells_x * cells_y
    ny = cells_y + 2

    @pl.loop(0, columns)
    def _(column):
        outs, counts = compress_cells(halo_ref, column // cells_y, column % cells_y, ny)
        for k in range(18):
            packed_ref[column * 36 + 2 * k] = outs[k]
            packed_ref[column * 36 + 2 * k + 1] = pltpu.roll(outs[k], 7, 0)
        for cz in (0, 1):
            count_vmem[pl.ds(column * 2 + cz, 1), :] = counts[cz]

    copy = pltpu.make_async_copy(count_vmem, count_ref, sem)
    copy.start()
    copy.wait()

    @pl.loop(0, columns)
    def _(column):
        lengths = merge_cells(packed_ref, count_ref, list_ref, column)
        for cz in (0, 1):
            length_ref[column * 2 + cz] = (lengths[cz] + (WIDE * LANES - 1)) >> int(math.log2(WIDE * LANES))

    @pl.loop(0, 2 * columns)
    def _(cell):
        column = cell // 2
        begin = (cell % 2) * SLOTS
        steps = length_ref[cell]
        blocks = (own_ref[cell] + DENSE_ROWS - 1) // DENSE_ROWS

        @pl.loop(0, blocks)
        def _(block):
            start = pl.multiple_of(begin + block * DENSE_ROWS, DENSE_ROWS)
            centers = [
                jnp.concatenate([center_ref[column, c, pl.ds(start, DENSE_ROWS), :]] * WIDE, axis=1) for c in range(3)
            ]

            def step(index, sums):
                tile = jnp.concatenate(
                    [list_ref[cell * TILES + index * WIDE + k] for k in range(WIDE)], axis=1
                )
                return (sums[0] + fold(pair_parts(centers, tile)[0]),)

            zero = jnp.zeros((DENSE_ROWS, LANES), jnp.float32)
            sums = lax.fori_loop(0, steps, step, (zero,))
            sum_ref[0, column, pl.ds(start, DENSE_ROWS), :] = sums[0]

    filled = jnp.concatenate(
        [placed_ref[c // cells_y, c % cells_y, 0:1] for c in range(columns)], axis=0
    ) < 0.5 * FAR
    density = jnp.concatenate([lane_sums(sum_ref[0, c]) for c in range(columns)], axis=0)
    embed_value, embed_slope = embedding(jnp.where(filled, density, 0.0))
    slope = jnp.where(filled, embed_slope, 0.0)
    for c in range(columns):
        slope_ref[c // cells_y, c % cells_y] = slope[c : c + 1]
    embed_ref[...] = embed_value


def force_kernel(
    own_ref,
    placed_ref,
    embed_ref,
    halo_ref,
    slope_center,
    center_ref,
    packed_in,
    list_ref,
    count_vmem,
    force_ref,
    energy_ref,
    packed_ref,
    slope_list,
    count_ref,
    length_ref,
    sum_ref,
    sem,
):
    cells_x, cells_y = placed_ref.shape[:2]
    columns = cells_x * cells_y
    ny = cells_y + 2
    copy = pltpu.make_async_copy(count_vmem, count_ref, sem)
    copy.start()
    filled = jnp.concatenate(
        [placed_ref[c // cells_y, c % cells_y, 0:1] for c in range(columns)], axis=0
    ) < 0.5 * FAR

    @pl.loop(0, columns)
    def _(column):
        cx, cy = (column // cells_y, column % cells_y)
        for k in range(9):
            value = halo_ref[(cx + k // 3) * ny + cy + k % 3]
            for cz in (0, 1):
                at = column * 36 + 18 * cz + 2 * k
                index = packed_in[at].astype(jnp.int32) & (LANES - 1)
                taken = jnp.take_along_axis(value, index, axis=1, mode="promise_in_bounds")
                packed_ref[at] = taken
                packed_ref[at + 1] = pltpu.roll(taken, 7, 0)

    copy.wait()

    @pl.loop(0, columns)
    def _(column):
        lengths = merge_cells(packed_ref, count_ref, slope_list, column)
        for cz in (0, 1):
            length_ref[column * 2 + cz] = (lengths[cz] + (WIDE * LANES - 1)) >> int(math.log2(WIDE * LANES))

    @pl.loop(0, 2 * columns)
    def _(cell):
        column = cell // 2
        begin = (cell % 2) * SLOTS
        steps = length_ref[cell]
        blocks = (own_ref[cell] + ROWS - 1) // ROWS

        @pl.loop(0, blocks)
        def _(block):
            start = pl.multiple_of(begin + block * ROWS, ROWS)
            centers = [
                jnp.concatenate([center_ref[column, c, pl.ds(start, ROWS), :]] * WIDE, axis=1) for c in range(3)
            ]
            slope_i = jnp.concatenate([slope_center[column, 0, pl.ds(start, ROWS), :]] * WIDE, axis=1)

            def step(index, sums):
                at = [cell * TILES + index * WIDE + k for k in range(WIDE)]
                tile = jnp.concatenate([list_ref[t] for t in at], axis=1)
                slope_j = jnp.concatenate([slope_list[t] for t in at], axis=1)[6:7]
                parts = pair_parts(centers, tile, slope_i + slope_j)
                return tuple(total + fold(part) for total, part in zip(sums, parts))

            zero = jnp.zeros((ROWS, LANES), jnp.float32)
            sums = lax.fori_loop(0, steps, step, (zero,) * 4)
            for k in range(4):
                sum_ref[k, column, pl.ds(start, ROWS), :] = sums[k]

    pair_sum = jnp.concatenate([lane_sums(sum_ref[0, c]) for c in range(columns)], axis=0)
    energy_ref[...] = jnp.where(filled, embed_ref[...] + 0.5 * pair_sum, 0.0)
    for k in range(3):
        total = jnp.concatenate([lane_sums(sum_ref[1 + k, c]) for c in range(columns)], axis=0)
        force_ref[k] = jnp.where(filled, total, 0.0)


def on_device(positions, counts):
    cells_x, cells_y, cells_z = counts.shape
    columns = cells_x * cells_y
    cells = columns * cells_z
    occupied = lax.broadcasted_iota(jnp.int32, (cells_x, cells_y, cells_z, SLOTS), 3) < counts[..., None]
    occupied = occupied.reshape(1, cells_x, cells_y, cells_z * SLOTS)
    placed = jnp.transpose(jnp.where(occupied, positions, FAR), (1, 2, 0, 3))
    sizes = {axis: lax.axis_size(axis) for axis in ("gx", "gy", "gz")}
    own = counts.reshape(cells)
    vmem = pl.BlockSpec(memory_space=pltpu.VMEM)
    smem = pl.BlockSpec(memory_space=pltpu.SMEM)
    f32 = jnp.float32
    shape = jax.ShapeDtypeStruct
    params = pltpu.CompilerParams(vmem_limit_bytes=24 * 1024 * 1024)
    halo, center = call_exchange(sizes, placed, 0)
    work = [
        pltpu.SMEM((cells, LANES), jnp.int32),
        pltpu.SMEM((cells,), jnp.int32),
        pltpu.VMEM((4, columns, LANES, LANES), f32),
        pltpu.SemaphoreType.DMA,
    ]
    saved = (
        shape((cells * 18, 8, LANES), f32),
        shape((cells * TILES, 8, LANES), f32),
        shape((cells, LANES), jnp.int32),
    )
    slope, embed, *kept = pl.pallas_call(
        density_kernel,
        out_shape=(shape((cells_x, cells_y, 1, LANES), f32), shape((columns, LANES), f32)) + saved,
        in_specs=[smem, vmem, vmem, vmem],
        out_specs=(vmem,) * 5,
        scratch_shapes=work,
        compiler_params=params,
        name="density",
    )(own, placed, halo, center)
    halo, slope_center = call_exchange(sizes, slope, 1)
    forces, energy = pl.pallas_call(
        force_kernel,
        out_shape=(shape((3, columns, LANES), f32), shape((columns, LANES), f32)),
        in_specs=[smem] + [vmem] * 8,
        out_specs=(vmem, vmem),
        scratch_shapes=[
            pltpu.VMEM((cells * 18, 8, LANES), f32),
            pltpu.VMEM((cells * TILES, 8, LANES), f32),
        ]
        + work,
        compiler_params=params,
        name="forces",
    )(own, placed, embed, halo, slope_center, center, *kept)
    return (
        forces.reshape(3, cells_x, cells_y, cells_z * SLOTS),
        energy.reshape(cells_x, cells_y, cells_z * SLOTS),
    )


def solution(mesh):
    return jax.shard_map(
        on_device,
        mesh=mesh,
        in_specs=(P(None, "gx", "gy", "gz"), P("gx", "gy", "gz")),
        out_specs=(P(None, "gx", "gy", "gz"), P("gx", "gy", "gz")),
        check_vma=False,
    )
```
